8 devices in a mesh: dp: 1 (over z), cols: 2 (over y), rows: 4 (over x, core).
Axes of the slice: x: 2, y: 2, z: 1, core: 2. Of those that a mesh axis runs over, the one named last changes fastest.
Arguments:
- frames: bfloat16 [32, 2, 128, 96, 4], P(None, 'dp', 'rows', 'cols')
- w_in: bfloat16 [3, 3, 4, 256], replicated
- w_rec: bfloat16 [3, 3, 64, 256], replicated
- gate_bias: float32 [256], replicated
- h_init: bfloat16 [2, 128, 96, 64], P('dp', 'rows', 'cols')
- c_init: float32 [2, 128, 96, 64], P('dp', 'rows', 'cols')
Outputs:
- output 1: bfloat16 [32, 2, 128, 96, 64], P(None, 'dp', 'rows', 'cols')
- output 2: float32 [2, 128, 96, 64], P('dp', 'rows', 'cols')
All inputs are finite; a program needn't handle non-finite values.
Results may differ from the reference program's by a relative error of at most 0.00440778.
Values are sent between devices in bfloat16 or wider.
A program may use at most 1 GiB of HBM per device.

```python
import jax
import jax.numpy as jnp
from jax import lax

STEPS = 32
BATCH = 2
GRID_H = 128
GRID_W = 96
C_IN = 4
C_HID = 64

CONV_DIMS = ("NHWC", "HWIO", "NHWC")


def setup_inputs(seed: int = 0, part: int = 0) -> dict:
    part_key = jax.random.fold_in(jax.random.key(seed), part)
    k_frames, k_hid, k_cell = jax.random.split(part_key, 3)
    k_win, k_wrec, k_bias = jax.random.split(jax.random.key(seed + 1), 3)
    frames = jax.random.normal(k_frames, (STEPS, BATCH, GRID_H, GRID_W, C_IN), jnp.float32)
    w_in = jax.random.normal(k_win, (3, 3, C_IN, 4 * C_HID), jnp.float32) * (9 * C_IN) ** -0.5
    w_rec = jax.random.normal(k_wrec, (3, 3, C_HID, 4 * C_HID), jnp.float32) * (2.0 * (9 * C_HID) ** -0.5)
    forget_shift = jnp.concatenate([jnp.zeros((C_HID,), jnp.float32), jnp.ones((C_HID,), jnp.float32), jnp.zeros((2 * C_HID,), jnp.float32)])
    gate_bias = 0.5 * jax.random.normal(k_bias, (4 * C_HID,), jnp.float32) + forget_shift
    h_init = 0.5 * jax.random.normal(k_hid, (BATCH, GRID_H, GRID_W, C_HID), jnp.float32)
    c_init = jax.random.normal(k_cell, (BATCH, GRID_H, GRID_W, C_HID), jnp.float32)
    return {
        "frames": frames.astype(jnp.bfloat16),
        "w_in": w_in.astype(jnp.bfloat16),
        "w_rec": w_rec.astype(jnp.bfloat16),
        "gate_bias": gate_bias,
        "h_init": h_init.astype(jnp.bfloat16),
        "c_init": c_init,
    }


def conv_same(operand, kernel):
    return lax.conv_general_dilated(operand.astype(jnp.float32), kernel, (1, 1), "SAME", dimension_numbers=CONV_DIMS)


def reference(frames, w_in, w_rec, gate_bias, h_init, c_init):
    w_in32 = w_in.astype(jnp.float32)
    w_rec32 = w_rec.astype(jnp.float32)

    def time_step(carry_in, frame_t):
        h_prev, c_prev = carry_in
        gate_pre = conv_same(frame_t, w_in32) + conv_same(h_prev, w_rec32) + gate_bias
        gate_i, gate_f, gate_o, gate_g = jnp.split(gate_pre, 4, axis=-1)
        c_next = jax.nn.sigmoid(gate_f) * c_prev + jax.nn.sigmoid(gate_i) * jnp.tanh(gate_g)
        h_next = (jax.nn.sigmoid(gate_o) * jnp.tanh(c_next)).astype(jnp.bfloat16)
        return (h_next, c_next), h_next

    (h_last, c_last), hidden_seq = lax.scan(time_step, (h_init, c_init), frames)
    return hidden_seq, c_last
```

```python
import jax
import jax.numpy as jnp
from jax import lax
from jax.experimental import pallas as pl
from jax.experimental.pallas import tpu as pltpu
from jax.sharding import PartitionSpec as P

MESH = pl.DeviceIdType.MESH
F32, BF16 = jnp.float32, jnp.bfloat16

STEPS = 32
SAMPLES = 2
TILE_H = 32
TILE_W = 48
C_IN = 4
C_HID = 64
ROUND = 4
ROUNDS = STEPS // ROUND
EXT = 8
PITCH = TILE_W + EXT
ROW = SAMPLES * PITCH
ROWS = TILE_H + 2 * ROUND
CELLS = ROWS * ROW
PAD = 8
LANES = 128
EDGE = ROUND * SAMPLES * TILE_W
HALF = LANES // 2


def chunk_rows(count):
    for rows in (9, 8, 19, 17):
        if count % rows == 0:
            return rows
    raise ValueError(count)


def kernel(frames_ref, state_ref, w_ref, bias_ref, seq_ref, c_out_ref,
           h_buf, c_buf, g_buf, a_buf, out_buf, gain_buf,
           up_buf, down_buf, edge_buf, from_up, from_down, from_edge,
           send_sem, recv_sem, out_sem):
    row = lax.axis_index("rows")
    col = lax.axis_index("cols")
    has_up = row > 0
    has_down = row < lax.axis_size("rows") - 1
    is_left = col == 0
    other = 1 - col

    own_at = jnp.where(is_left, 0, EXT)
    edge_at = jnp.where(is_left, TILE_W - EXT, EXT)
    halo_at = jnp.where(is_left, TILE_W, 0)

    lane = lax.broadcasted_iota(jnp.int32, (EXT, LANES), 1)
    cell = lax.broadcasted_iota(jnp.int32, (EXT, LANES), 0)
    low = lane < HALF
    halo_cell = jnp.where(is_left, (cell < ROUND).astype(F32), (cell >= EXT - ROUND).astype(F32))

    def low_mask(cells):
        return lax.broadcasted_iota(jnp.int32, (cells, LANES), 1) < HALF

    zero_h = jnp.zeros((ROW, LANES), F32)
    zero_a = jnp.zeros((ROW, 2 * LANES), BF16)
    pad = jnp.zeros((PAD, LANES), F32)
    for buf in (h_buf, c_buf, g_buf):
        buf[pl.ds(0, PAD), :] = pad
        buf[pl.ds(PAD + CELLS, PAD), :] = pad

    @pl.loop(0, ROWS)
    def _(y):
        at = pl.multiple_of(y * ROW, ROW)
        h_buf[pl.ds(PAD + at, ROW), :] = zero_h
        c_buf[pl.ds(PAD + at, ROW), :] = zero_h
        g_buf[pl.ds(PAD + at, ROW), :] = zero_h
        a_buf[pl.ds(at, ROW), :] = zero_a
        for slot in range(3):
            from_edge[slot, pl.ds(pl.multiple_of(y * EXT, EXT), EXT), :] = pad

    gain = jnp.where(low, 0.5, 1.0)
    shift = jnp.where(low, 0.5, 0.0)
    for s in range(SAMPLES):
        for v in range(PITCH // EXT):
            at = s * PITCH + v * EXT
            is_halo = halo_at == v * EXT
            keep = jnp.where(is_halo, halo_cell, 1.0)
            gain_buf[0, pl.ds(at, EXT), :] = gain * keep
            gain_buf[1, pl.ds(at, EXT), :] = shift * keep

    barrier = pltpu.get_barrier_semaphore()

    def greet(target):
        pl.semaphore_signal(barrier, inc=1, device_id=target, device_id_type=MESH)

    greet({"cols": other})

    @pl.when(has_up)
    def _():
        greet({"rows": row - 1})
        greet({"rows": row - 1, "cols": other})

    @pl.when(has_down)
    def _():
        greet({"rows": row + 1})
        greet({"rows": row + 1, "cols": other})

    pl.semaphore_wait(barrier, 1 + 2 * has_up.astype(jnp.int32) + 2 * has_down.astype(jnp.int32))

    def copies(slot):
        def copy(src, dst, index, target):
            return pltpu.make_async_remote_copy(
                src_ref=src, dst_ref=dst, send_sem=send_sem.at[slot, index],
                recv_sem=recv_sem.at[slot, index], device_id=target, device_id_type=MESH)

        edge = edge_buf.at[slot]
        halo = from_edge.at[slot]
        corner = ROUND * EXT
        own = TILE_H * EXT
        return (
            copy(up_buf.at[slot], from_down.at[slot], 0, {"rows": row - 1}),
            copy(down_buf.at[slot], from_up.at[slot], 1, {"rows": row + 1}),
            copy(edge, halo.at[pl.ds(corner, own)], 2, {"cols": other}),
            copy(edge.at[pl.ds(0, corner)], halo.at[pl.ds(corner + own, corner)], 3, {"rows": row - 1, "cols": other}),
            copy(edge.at[pl.ds(own - corner, corner)], halo.at[pl.ds(0, corner)], 4, {"rows": row + 1, "cols": other}),
        )

    def send(slot, read):
        for r in range(ROUND):
            for s in range(SAMPLES):
                to = pl.ds((r * SAMPLES + s) * TILE_W, TILE_W)
                at = pl.multiple_of((ROUND + r) * ROW + s * PITCH + own_at, EXT)
                up_buf[slot, to, :] = read(at, TILE_W)
                at = pl.multiple_of((TILE_H + r) * ROW + s * PITCH + own_at, EXT)
                down_buf[slot, to, :] = read(at, TILE_W)

        @pl.loop(0, TILE_H)
        def _(y):
            first = read(pl.multiple_of((ROUND + y) * ROW + edge_at, EXT), EXT)
            second = read(pl.multiple_of((ROUND + y) * ROW + PITCH + edge_at, EXT), EXT)
            first = jnp.where(is_left, pltpu.roll(first, EXT // 2, 0), first)
            second = jnp.where(is_left, second, pltpu.roll(second, EXT // 2, 0))
            edge_buf[slot, pl.ds(pl.multiple_of(y * EXT, EXT), EXT), :] = jnp.where(cell < EXT // 2, first, second)

        up, down, across, across_up, across_down = copies(slot)
        across.start()

        @pl.when(has_up)
        def _():
            up.start()
            across_up.start()

        @pl.when(has_down)
        def _():
            down.start()
            across_down.start()

    def receive(slot, write):
        up, down, across, across_up, across_down = copies(slot)
        across.wait_send()
        across.wait_recv()

        @pl.when(has_up)
        def _():
            up.wait_send()
            across_up.wait_send()
            down.wait_recv()
            across_down.wait_recv()
            for r in range(ROUND):
                for s in range(SAMPLES):
                    frm = pl.ds((r * SAMPLES + s) * TILE_W, TILE_W)
                    write(pl.multiple_of(r * ROW + s * PITCH + own_at, EXT), from_up[slot, frm, :])

        @pl.when(has_down)
        def _():
            down.wait_send()
            across_down.wait_send()
            up.wait_recv()
            across_up.wait_recv()
            for r in range(ROUND):
                for s in range(SAMPLES):
                    frm = pl.ds((r * SAMPLES + s) * TILE_W, TILE_W)
                    write(pl.multiple_of((ROUND + TILE_H + r) * ROW + s * PITCH + own_at, EXT), from_down[slot, frm, :])

        @pl.loop(0, ROWS)
        def _(y):
            got = from_edge[slot, pl.ds(pl.multiple_of(y * EXT, EXT), EXT), :]
            turned = pltpu.roll(got, EXT // 2, 0)
            write(pl.multiple_of(y * ROW + halo_at, EXT), jnp.where(is_left, got, turned) * halo_cell)
            write(pl.multiple_of(y * ROW + PITCH + halo_at, EXT), jnp.where(is_left, turned, got) * halo_cell)

    def read_frames(at, cells):
        return g_buf[pl.ds(PAD + at, cells), :]

    def write_frames(at, value):
        g_buf[pl.ds(PAD + at, value.shape[0]), :] = value

    def read_state(at, cells):
        return jnp.where(low_mask(cells), h_buf[pl.ds(PAD + at, cells), :], c_buf[pl.ds(PAD + at, cells), :])

    def write_state(at, value):
        cells = value.shape[0]
        h_buf[pl.ds(PAD + at, cells), :] = value
        c_buf[pl.ds(PAD + at, cells), :] = jnp.where(low_mask(cells), pltpu.roll(value, HALF, 1), value)

    @pl.loop(0, TILE_H)
    def _(y):
        for s in range(SAMPLES):
            at = pl.multiple_of((ROUND + y) * ROW + s * PITCH + own_at, EXT)
            write_frames(at, frames_ref[y, s, :, :].astype(F32))
            write_state(at, state_ref[y, s, :, :])

    send(2, read_frames)
    send(0, read_state)
    receive(2, write_frames)

    def build(y, with_frames, turn):
        at = pl.multiple_of(y * ROW, ROW)
        mine = h_buf[pl.ds(PAD + at, ROW), :]
        before = h_buf[pl.ds(PAD - 1 + at, ROW), :]
        after = h_buf[pl.ds(PAD + 1 + at, ROW), :]
        low_row = low_mask(ROW)
        a_buf[pl.ds(at, ROW), 0:LANES] = jnp.where(low_row, mine, pltpu.roll(before, HALF, 1)).astype(BF16)
        if with_frames:
            lane_row = lax.broadcasted_iota(jnp.int32, (ROW, LANES), 1)
            f_mine = pltpu.roll(g_buf[pl.ds(PAD + at, ROW), :], turn(80), 1)
            f_before = pltpu.roll(g_buf[pl.ds(PAD - 1 + at, ROW), :], turn(64), 1)
            f_after = pltpu.roll(g_buf[pl.ds(PAD + 1 + at, ROW), :], turn(96), 1)
            f = jnp.where(lane_row < 80, f_before, jnp.where(lane_row < 96, f_mine, f_after))
            a_buf[pl.ds(at, ROW), LANES:2 * LANES] = jnp.where(low_row, after, f).astype(BF16)
        else:
            a_buf[pl.ds(at, ROW), LANES:LANES + HALF] = after[:, 0:HALF].astype(BF16)

    def advance(y, rows, step, slot):
        at = pl.multiple_of(y * ROW, ROW)
        gates = jnp.zeros((rows * ROW, 2 * LANES), F32)
        for dy in range(3):
            left = a_buf[pl.ds(pl.multiple_of(at + (dy - 1) * ROW, ROW), rows * ROW), :]
            gates = gates + jnp.dot(left, w_ref[step, dy, :, :], preferred_element_type=F32)
        low_row = low_mask(ROW)
        for r in range(rows):
            part = slice(r * ROW, (r + 1) * ROW)
            here = pl.ds(PAD + at + r * ROW, ROW)
            first = jnp.tanh(gates[part, 0:LANES] + bias_ref[0:1, :])
            second = jnp.tanh(gates[part, LANES:] + bias_ref[1:2, :])
            mixed = (0.5 * first + 0.5) * jnp.where(low_row, c_buf[here, :], second)
            c_next = mixed + pltpu.roll(mixed, HALF, 1)
            c_buf[here, :] = c_next
            h_next = (second * gain_buf[0, :, :] + gain_buf[1, :, :]) * jnp.tanh(c_next)
            h_buf[here, :] = h_next
            for s in range(SAMPLES):
                own = jnp.where(is_left, h_next[s * PITCH:s * PITCH + TILE_W, :], h_next[s * PITCH + EXT:(s + 1) * PITCH, :])
                out_buf[slot, s, y + r, :, :] = own[:, 0:C_HID].astype(BF16)

    def out_copy(t, slot):
        return pltpu.make_async_copy(
            out_buf.at[slot, :, pl.ds(ROUND, TILE_H)], seq_ref.at[t], out_sem.at[slot])

    @pl.loop(0, ROUNDS)
    def _(n):
        receive(n % 2, write_state)

        def turn(lane_to):
            return lax.rem(lane_to + LANES - ROUND * C_IN * n, LANES)

        for j in range(1, ROUND + 1):
            step = j - 1
            t = ROUND * n + step
            slot = step % 2

            @pl.when(t >= 2)
            def _():
                out_copy(t - 2, slot).wait()

            def build_own(y):
                build(y, j == 1, turn)

            for y in range(j - 1, ROUND):
                pl.when(has_up)(lambda y=y: build_own(y))
            for y in range(ROUND + TILE_H, ROWS - j + 1):
                pl.when(has_down)(lambda y=y: build_own(y))
            pl.loop(ROUND, ROUND + TILE_H)(build_own)

            count = ROWS - 2 * j
            rows = chunk_rows(count)
            pl.loop(0, count // rows)(lambda i: advance(j + i * rows, rows, step, slot))
            out_copy(t, slot).start()

        @pl.when(n < ROUNDS - 1)
        def _():
            send((n + 1) % 2, read_state)

    for t in (STEPS - 2, STEPS - 1):
        out_copy(t, t % 2).wait()

    @pl.loop(0, TILE_H)
    def _(y):
        for s in range(SAMPLES):
            at = pl.multiple_of((ROUND + y) * ROW + s * PITCH + own_at, EXT)
            c_out_ref[s, y, :, :] = c_buf[pl.ds(PAD + at, TILE_W), 0:C_HID]


def pack_weights(w_in, w_rec):
    def gates(w):
        i, f, o, g = jnp.split(w, 4, axis=-1)
        half = jnp.asarray(0.5, w.dtype)
        return jnp.concatenate([f * half, i * half, o * half, g], axis=-1)

    rec = gates(w_rec)
    rec = jnp.concatenate([rec[:, 1], rec[:, 0], rec[:, 2]], axis=1)
    inp = gates(w_in)
    rest = LANES - HALF - 3 * ROUND * C_IN
    packed = []
    for step in range(ROUND):
        spread = jnp.pad(inp, ((0, 0), (0, 0), (step * C_IN, (ROUND - 1 - step) * C_IN), (0, 0)))
        spread = spread.reshape(3, 3 * ROUND * C_IN, 4 * C_HID)
        packed.append(jnp.concatenate([rec, jnp.pad(spread, ((0, 0), (0, rest), (0, 0)))], axis=1))
    return jnp.stack(packed)


def pack_bias(bias):
    i, f, o, g = jnp.split(bias, 4)
    return jnp.stack([jnp.concatenate([f, i]) * 0.5, jnp.concatenate([o * 0.5, g])])


def solution(mesh):
    assert mesh.shape["cols"] == 2
    seq_spec = P(None, "dp", "rows", "cols", None)
    state_spec = P("dp", "rows", "cols", None)

    def local_run(frames, w_in, w_rec, gate_bias, h_init, c_init):
        frames_cells = frames.transpose(2, 1, 3, 0, 4).reshape(TILE_H, SAMPLES, TILE_W, STEPS * C_IN)
        state = jnp.concatenate([h_init.astype(F32), c_init], axis=-1).transpose(1, 0, 2, 3)
        vmem = pl.BlockSpec(memory_space=pltpu.VMEM)
        return pl.pallas_call(
            kernel,
            out_shape=(
                jax.ShapeDtypeStruct((STEPS, SAMPLES, TILE_H, TILE_W, C_HID), BF16),
                jax.ShapeDtypeStruct((SAMPLES, TILE_H, TILE_W, C_HID), F32),
            ),
            in_specs=[vmem] * 4,
            out_specs=(pl.BlockSpec(memory_space=pl.ANY), vmem),
            scratch_shapes=[
                pltpu.VMEM((CELLS + 2 * PAD, LANES), F32),
                pltpu.VMEM((CELLS + 2 * PAD, LANES), F32),
                pltpu.VMEM((CELLS + 2 * PAD, LANES), F32),
                pltpu.VMEM((CELLS, 2 * LANES), BF16),
                pltpu.VMEM((2, SAMPLES, ROWS, TILE_W, C_HID), BF16),
                pltpu.VMEM((2, ROW, LANES), F32),
                pltpu.VMEM((3, EDGE, LANES), F32),
                pltpu.VMEM((3, EDGE, LANES), F32),
                pltpu.VMEM((3, TILE_H * EXT, LANES), F32),
                pltpu.VMEM((3, EDGE, LANES), F32),
                pltpu.VMEM((3, EDGE, LANES), F32),
                pltpu.VMEM((3, ROWS * EXT, LANES), F32),
                pltpu.SemaphoreType.DMA((3, 5)),
                pltpu.SemaphoreType.DMA((3, 5)),
                pltpu.SemaphoreType.DMA((2,)),
            ],
            compiler_params=pltpu.CompilerParams(
                collective_id=0, has_side_effects=True, vmem_limit_bytes=48 * 1024 * 1024),
            name="convlstm",
        )(frames_cells, state, pack_weights(w_in, w_rec), pack_bias(gate_bias))

    return jax.shard_map(
        local_run, mesh=mesh, in_specs=(seq_spec, P(), P(), P(), state_spec, state_spec),
        out_specs=(seq_spec, state_spec), check_vma=False)
```

```python
import jax
import jax.numpy as jnp
from jax import lax
from jax.experimental import pallas as pl
from jax.experimental.pallas import tpu as pltpu
from jax.sharding import PartitionSpec as P

MESH = pl.DeviceIdType.MESH
F32, BF16 = jnp.float32, jnp.bfloat16

STEPS = 32
SAMPLES = 2
TILE_H = 32
TILE_W = 48
C_IN = 4
C_HID = 64
ROUND = 4
ROUNDS = STEPS // ROUND
EXT = 8
WIDE = TILE_W + EXT
PITCH = 64
ROWS = TILE_H + 2 * ROUND
LANES = 128
HALF = LANES // 2
STRIP = ROUND * TILE_W
EDGE = TILE_H // 2 * EXT
EDGE_HALO = ROWS // 2 * EXT
CORNER = ROUND // 2 * EXT
SLOTS = 3 * SAMPLES


def kernel(frames_ref, h_ref, c_ref, w_ref, bias_ref, seq_ref, c_out_ref,
           h_buf, c_buf, g_buf, a_buf, out_buf,
           up_buf, down_buf, edge_buf, from_up, from_down, from_edge,
           send_sem, recv_sem, out_sem):
    row = lax.axis_index("rows")
    col = lax.axis_index("cols")
    has_up = row > 0
    has_down = row < lax.axis_size("rows") - 1
    is_left = col == 0
    other = 1 - col

    own_at = jnp.where(is_left, 0, EXT)
    edge_at = jnp.where(is_left, TILE_W - EXT, EXT)
    halo_at = jnp.where(is_left, TILE_W, 0)
    up_keep = has_up.astype(F32)
    down_keep = has_down.astype(F32)

    def lane_of(cells):
        return lax.broadcasted_iota(jnp.int32, (cells, LANES), 1)

    def low(cells):
        return lane_of(cells) < HALF

    def aligned(at):
        return pl.multiple_of(at, EXT)

    zero = jnp.zeros((WIDE, LANES), F32)
    tail = jnp.zeros((PITCH - WIDE, LANES), F32)

    @pl.loop(0, ROWS)
    def _(y):
        for s in range(SAMPLES):
            at = pl.ds(aligned(y * WIDE), WIDE)
            h_buf[s, at, :] = zero
            c_buf[s, at, :] = zero
            g_buf[s, at, :] = zero
        a_buf[1, pl.ds(pl.multiple_of(y * PITCH, PITCH), PITCH), 0:LANES] = jnp.zeros((PITCH, LANES), BF16)

    for slot in range(SLOTS):
        for at in (0, EDGE_HALO - CORNER):
            from_edge[slot, pl.ds(at, CORNER), :] = jnp.zeros((CORNER, LANES), F32)

    barrier = pltpu.get_barrier_semaphore()

    def greet(target):
        pl.semaphore_signal(barrier, inc=1, device_id=target, device_id_type=MESH)

    greet({"cols": other})

    @pl.when(has_up)
    def _():
        greet({"rows": row - 1})
        greet({"rows": row - 1, "cols": other})

    @pl.when(has_down)
    def _():
        greet({"rows": row + 1})
        greet({"rows": row + 1, "cols": other})

    pl.semaphore_wait(barrier, 1 + 2 * has_up.astype(jnp.int32) + 2 * has_down.astype(jnp.int32))

    def copies(slot):
        def copy(src, dst, index, target):
            return pltpu.make_async_remote_copy(
                src_ref=src, dst_ref=dst, send_sem=send_sem.at[slot, index],
                recv_sem=recv_sem.at[slot, index], device_id=target, device_id_type=MESH)

        edge = edge_buf.at[slot]
        halo = from_edge.at[slot]
        return (
            copy(up_buf.at[slot], from_down.at[slot], 0, {"rows": row - 1}),
            copy(down_buf.at[slot], from_up.at[slot], 1, {"rows": row + 1}),
            copy(edge, halo.at[pl.ds(CORNER, EDGE)], 2, {"cols": other}),
            copy(edge.at[pl.ds(0, CORNER)], halo.at[pl.ds(CORNER + EDGE, CORNER)], 3, {"rows": row - 1, "cols": other}),
            copy(edge.at[pl.ds(EDGE - CORNER, CORNER)], halo.at[pl.ds(0, CORNER)], 4, {"rows": row + 1, "cols": other}),
        )

    cell = lax.broadcasted_iota(jnp.int32, (EXT, LANES), 0)

    def send(slot, read):
        up, down, across, across_up, across_down = copies(slot)

        @pl.loop(0, TILE_H // 2, unroll=8)
        def _(y):
            at = (ROUND + 2 * y) * WIDE + edge_at
            first = read(aligned(at), EXT)
            second = read(aligned(at + WIDE), EXT)
            first = jnp.where(is_left, pltpu.roll(first, EXT // 2, 0), first)
            second = jnp.where(is_left, second, pltpu.roll(second, EXT // 2, 0))
            edge_buf[slot, pl.ds(aligned(y * EXT), EXT), :] = jnp.where(cell < EXT // 2, first, second)

        across.start()
        for r in range(ROUND):
            up_buf[slot, pl.ds(r * TILE_W, TILE_W), :] = read(aligned((ROUND + r) * WIDE + own_at), TILE_W)
            down_buf[slot, pl.ds(r * TILE_W, TILE_W), :] = read(aligned((TILE_H + r) * WIDE + own_at), TILE_W)

        @pl.when(has_up)
        def _():
            up.start()
            across_up.start()

        @pl.when(has_down)
        def _():
            down.start()
            across_down.start()

    def receive(slot, write):
        up, down, across, across_up, across_down = copies(slot)

        @pl.when(has_up)
        def _():
            up.wait_send()
            across_up.wait_send()
            down.wait_recv()
            across_down.wait_recv()
            for r in range(ROUND):
                write(aligned(r * WIDE + own_at), from_up[slot, pl.ds(r * TILE_W, TILE_W), :])

        @pl.when(has_down)
        def _():
            down.wait_send()
            across_down.wait_send()
            up.wait_recv()
            across_up.wait_recv()
            for r in range(ROUND):
                write(aligned((ROUND + TILE_H + r) * WIDE + own_at), from_down[slot, pl.ds(r * TILE_W, TILE_W), :])

        across.wait_send()
        across.wait_recv()

        @pl.loop(0, ROWS // 2, unroll=10)
        def _(y):
            got = from_edge[slot, pl.ds(aligned(y * EXT), EXT), :]
            turned = pltpu.roll(got, EXT // 2, 0)
            at = 2 * y * WIDE + halo_at
            write(aligned(at), jnp.where(is_left, got, turned))
            write(aligned(at + WIDE), jnp.where(is_left, turned, got))

    def frames_io(s):
        def read(at, cells):
            return g_buf[s, pl.ds(at, cells), :]

        def write(at, value):
            g_buf[s, pl.ds(at, value.shape[0]), :] = value

        return read, write

    def state_io(s):
        def read(at, cells):
            return jnp.where(low(cells), h_buf[s, pl.ds(at, cells), :], c_buf[s, pl.ds(at, cells), :])

        def write(at, value):
            cells = value.shape[0]
            h_buf[s, pl.ds(at, cells), :] = value
            c_buf[s, pl.ds(at, cells), :] = jnp.where(low(cells), pltpu.roll(value, HALF, 1), value)

        return read, write

    def frames_slot(s):
        return 2 * SAMPLES + s

    for s in range(SAMPLES):
        @pl.loop(0, TILE_H, unroll=2)
        def _(y):
            at = aligned((ROUND + y) * WIDE + own_at)
            frames_io(s)[1](at, frames_ref[s, y, :, :].astype(F32))

        send(frames_slot(s), frames_io(s)[0])

        @pl.loop(0, TILE_H, unroll=2)
        def _(y):
            at = aligned((ROUND + y) * WIDE + own_at)
            state = jnp.concatenate([h_ref[s, y, :, :].astype(F32), c_ref[s, y, :, :]], axis=1)
            state_io(s)[1](at, state)

        send(2 * s, state_io(s)[0])

    def build(s, n, y):
        at = pl.ds(aligned(y * WIDE), WIDE)
        frames = pltpu.roll(g_buf[s, at, :], lax.rem(HALF + LANES - ROUND * C_IN * n, LANES), 1)
        here = jnp.concatenate([jnp.where(low(WIDE), h_buf[s, at, :], frames), tail])
        before = pltpu.roll(here, 1, 0)
        after = pltpu.roll(here, PITCH - 1, 0)
        lane = lane_of(PITCH)
        first = jnp.where(low(PITCH), here, pltpu.roll(before, HALF, 1))
        second = jnp.where(lane < 80, after, jnp.where(lane < 96, pltpu.roll(here, 16, 1), pltpu.roll(before, 32, 1)))
        second = second.astype(BF16)
        to = pl.ds(pl.multiple_of(y * PITCH, PITCH), PITCH)
        a_buf[0, to, 0:LANES] = first.astype(BF16)
        a_buf[0, to, LANES:2 * LANES] = second
        a_buf[1, to, LANES:2 * LANES] = second

    def advance(s, j, slot):
        step = j - 1
        old, new = step % 2, 1 - step % 2
        count = ROWS - 2 * j
        gates = None
        for dy in range(3):
            left = a_buf[old, pl.ds((j + dy - 1) * PITCH, count * PITCH), :]
            term = jnp.dot(left, w_ref[step, dy, :, :], preferred_element_type=F32)
            gates = term if gates is None else gates + term
        gain = jnp.where(low(1), 0.5, 1.0)
        shift = jnp.where(low(1), 0.5, 0.0)
        for r in range(count):
            y = j + r
            part = slice(r * PITCH, r * PITCH + WIDE)
            here = pl.ds(y * WIDE, WIDE)
            first = jnp.tanh(gates[part, 0:LANES] + bias_ref[0:1, :])
            second = jnp.tanh(gates[part, LANES:] + bias_ref[1:2, :])
            mixed = (0.5 * first + 0.5) * jnp.where(low(WIDE), c_buf[s, here, :], second)
            c_next = mixed + pltpu.roll(mixed, HALF, 1)
            c_buf[s, here, :] = c_next
            h_next = (second * gain + shift) * jnp.tanh(c_next)
            if y < ROUND:
                h_next = h_next * up_keep
            elif y >= ROUND + TILE_H:
                h_next = h_next * down_keep
            else:
                own = jnp.where(is_left, h_next[0:TILE_W, :], h_next[EXT:WIDE, :])
                out_buf[slot, y - ROUND, :, :] = own[:, 0:C_HID].astype(BF16)
            if j == ROUND:
                h_buf[s, here, :] = h_next
            else:
                wide = jnp.concatenate([h_next, tail])
                before = pltpu.roll(wide, 1, 0)
                after = pltpu.roll(wide, PITCH - 1, 0)
                to = pl.ds(y * PITCH, PITCH)
                a_buf[new, to, 0:LANES] = jnp.where(low(PITCH), wide, pltpu.roll(before, HALF, 1)).astype(BF16)
                a_buf[new, to, LANES:LANES + HALF] = after[:, 0:HALF].astype(BF16)

    def out_copy(t, s, slot):
        return pltpu.make_async_copy(out_buf.at[slot], seq_ref.at[t, s], out_sem.at[slot])

    for s in range(SAMPLES):
        receive(frames_slot(s), frames_io(s)[1])

    @pl.loop(0, SAMPLES * ROUNDS)
    def _(turn):
        s = lax.rem(turn, SAMPLES)
        n = lax.div(turn, SAMPLES)
        receive(2 * s + lax.rem(n, 2), state_io(s)[1])

        @pl.loop(0, ROWS, unroll=4)
        def _(y):
            build(s, n, y)

        for j in range(1, ROUND + 1):
            slot = (j - 1) % 2
            if j <= 2:
                pl.when(turn > 0)(lambda: out_copy(0, 0, slot).wait())
            else:
                out_copy(0, 0, slot).wait()
            advance(s, j, slot)
            out_copy(ROUND * n + j - 1, s, slot).start()

        @pl.when(n < ROUNDS - 1)
        def _():
            send(2 * s + lax.rem(n + 1, 2), state_io(s)[0])

    for slot in range(2):
        out_copy(0, 0, slot).wait()

    for s in range(SAMPLES):
        @pl.loop(0, TILE_H, unroll=2)
        def _(y):
            at = aligned((ROUND + y) * WIDE + own_at)
            c_out_ref[s, y, :, :] = c_buf[s, pl.ds(at, TILE_W), 0:C_HID]


def pack_weights(w_in, w_rec):
    def gates(w):
        i, f, o, g = jnp.split(w, 4, axis=-1)
        half = jnp.asarray(0.5, w.dtype)
        return jnp.concatenate([f * half, i * half, o * half, g], axis=-1)

    rec = gates(w_rec)
    rec = jnp.concatenate([rec[:, 1], rec[:, 0], rec[:, 2]], axis=1)
    inp = gates(w_in)[:, ::-1]
    rest = LANES - HALF - 3 * ROUND * C_IN
    packed = []
    for step in range(ROUND):
        spread = jnp.pad(inp, ((0, 0), (0, 0), (step * C_IN, (ROUND - 1 - step) * C_IN), (0, 0)))
        spread = spread.reshape(3, 3 * ROUND * C_IN, 4 * C_HID)
        packed.append(jnp.concatenate([rec, jnp.pad(spread, ((0, 0), (0, rest), (0, 0)))], axis=1))
    return jnp.stack(packed)


def pack_bias(bias):
    i, f, o, g = jnp.split(bias, 4)
    return jnp.stack([jnp.concatenate([f, i]) * 0.5, jnp.concatenate([o * 0.5, g])])


def solution(mesh):
    assert mesh.shape["cols"] == 2
    seq_spec = P(None, "dp", "rows", "cols", None)
    state_spec = P("dp", "rows", "cols", None)

    def local_run(frames, w_in, w_rec, gate_bias, h_init, c_init):
        frames_cells = frames.transpose(1, 2, 3, 0, 4).reshape(SAMPLES, TILE_H, TILE_W, STEPS * C_IN)
        vmem = pl.BlockSpec(memory_space=pltpu.VMEM)
        return pl.pallas_call(
            kernel,
            out_shape=(
                jax.ShapeDtypeStruct((STEPS, SAMPLES, TILE_H, TILE_W, C_HID), BF16),
                jax.ShapeDtypeStruct((SAMPLES, TILE_H, TILE_W, C_HID), F32),
            ),
            in_specs=[vmem] * 5,
            out_specs=(pl.BlockSpec(memory_space=pl.ANY), vmem),
            scratch_shapes=[
                pltpu.VMEM((SAMPLES, ROWS * WIDE, LANES), F32),
                pltpu.VMEM((SAMPLES, ROWS * WIDE, LANES), F32),
                pltpu.VMEM((SAMPLES, ROWS * WIDE, LANES), F32),
                pltpu.VMEM((2, ROWS * PITCH, 2 * LANES), BF16),
                pltpu.VMEM((2, TILE_H, TILE_W, C_HID), BF16),
                pltpu.VMEM((SLOTS, STRIP, LANES), F32),
                pltpu.VMEM((SLOTS, STRIP, LANES), F32),
                pltpu.VMEM((SLOTS, EDGE, LANES), F32),
                pltpu.VMEM((SLOTS, STRIP, LANES), F32),
                pltpu.VMEM((SLOTS, STRIP, LANES), F32),
                pltpu.VMEM((SLOTS, EDGE_HALO, LANES), F32),
                pltpu.SemaphoreType.DMA((SLOTS, 5)),
                pltpu.SemaphoreType.DMA((SLOTS, 5)),
                pltpu.SemaphoreType.DMA((2,)),
            ],
            compiler_params=pltpu.CompilerParams(
                collective_id=0, has_side_effects=True, vmem_limit_bytes=48 * 1024 * 1024),
            name="convlstm",
        )(frames_cells, h_init, c_init, pack_weights(w_in, w_rec), pack_bias(gate_bias))

    return jax.shard_map(
        local_run, mesh=mesh, in_specs=(seq_spec, P(), P(), P(), state_spec, state_spec),
        out_specs=(seq_spec, state_spec), check_vma=False)
```

```python
import jax
import jax.numpy as jnp
from jax import lax
from jax.experimental import pallas as pl
from jax.experimental.pallas import tpu as pltpu
from jax.sharding import PartitionSpec as P

MESH = pl.DeviceIdType.MESH
F32, BF16 = jnp.float32, jnp.bfloat16

STEPS = 32
SAMPLES = 2
TILE_H = 32
TILE_W = 48
C_IN = 4
C_HID = 64
ROUND = 4
ROUNDS = STEPS // ROUND
EXT = 8
WIDE = TILE_W + EXT
PHASES = WIDE // 8
PITCH = 64
SUB_ROWS = 8
ROWS = TILE_H + 2 * ROUND
LANES = 128
HALF = LANES // 2
STRIP = ROUND * TILE_W
EDGE = TILE_H // 2 * EXT
EDGE_HALO = ROWS // 2 * EXT
CORNER = ROUND // 2 * EXT
SLOTS = 3 * SAMPLES


def kernel(frames_ref, h_ref, c_ref, w_ref, bias_ref, seq_ref, c_out_ref,
           s_buf, c_buf, g_buf, a_buf,
           up_buf, down_buf, edge_buf, from_up, from_down, from_edge,
           send_sem, recv_sem):
    row = lax.axis_index("rows")
    col = lax.axis_index("cols")
    has_up = row > 0
    has_down = row < lax.axis_size("rows") - 1
    is_left = col == 0
    other = 1 - col

    own_at = jnp.where(is_left, 0, EXT)
    edge_at = jnp.where(is_left, TILE_W - EXT, EXT)
    halo_at = jnp.where(is_left, TILE_W, 0)
    up_keep = has_up.astype(F32)
    down_keep = has_down.astype(F32)

    def lane_of(cells):
        return lax.broadcasted_iota(jnp.int32, (cells, LANES), 1)

    def low(cells):
        return lane_of(cells) < HALF

    def aligned(at):
        return pl.multiple_of(at, EXT)

    zero = jnp.zeros((WIDE, LANES), F32)
    tail = jnp.zeros((PITCH - WIDE, LANES), F32)

    @pl.loop(0, ROWS)
    def _(y):
        for s in range(SAMPLES):
            at = pl.ds(aligned(y * WIDE), WIDE)
            s_buf[s, at, :] = zero
            g_buf[s, at, :] = zero

    for slot in range(SLOTS):
        for at in (0, EDGE_HALO - CORNER):
            from_edge[slot, pl.ds(at, CORNER), :] = jnp.zeros((CORNER, LANES), F32)

    barrier = pltpu.get_barrier_semaphore()

    def greet(target):
        pl.semaphore_signal(barrier, inc=1, device_id=target, device_id_type=MESH)

    greet({"cols": other})

    @pl.when(has_up)
    def _():
        greet({"rows": row - 1})
        greet({"rows": row - 1, "cols": other})

    @pl.when(has_down)
    def _():
        greet({"rows": row + 1})
        greet({"rows": row + 1, "cols": other})

    pl.semaphore_wait(barrier, 1 + 2 * has_up.astype(jnp.int32) + 2 * has_down.astype(jnp.int32))

    def copies(slot):
        def copy(src, dst, index, target):
            return pltpu.make_async_remote_copy(
                src_ref=src, dst_ref=dst, send_sem=send_sem.at[slot, index],
                recv_sem=recv_sem.at[slot, index], device_id=target, device_id_type=MESH)

        edge = edge_buf.at[slot]
        halo = from_edge.at[slot]
        return (
            copy(up_buf.at[slot], from_down.at[slot], 0, {"rows": row - 1}),
            copy(down_buf.at[slot], from_up.at[slot], 1, {"rows": row + 1}),
            copy(edge, halo.at[pl.ds(CORNER, EDGE)], 2, {"cols": other}),
            copy(edge.at[pl.ds(0, CORNER)], halo.at[pl.ds(CORNER + EDGE, CORNER)], 3, {"rows": row - 1, "cols": other}),
            copy(edge.at[pl.ds(EDGE - CORNER, CORNER)], halo.at[pl.ds(0, CORNER)], 4, {"rows": row + 1, "cols": other}),
        )

    cell = lax.broadcasted_iota(jnp.int32, (EXT, LANES), 0)

    def send(slot, read):
        up, down, across, across_up, across_down = copies(slot)

        @pl.loop(0, TILE_H // 2, unroll=8)
        def _(y):
            at = (ROUND + 2 * y) * WIDE + edge_at
            first = read(aligned(at), EXT)
            second = read(aligned(at + WIDE), EXT)
            first = jnp.where(is_left, pltpu.roll(first, EXT // 2, 0), first)
            second = jnp.where(is_left, second, pltpu.roll(second, EXT // 2, 0))
            edge_buf[slot, pl.ds(aligned(y * EXT), EXT), :] = jnp.where(cell < EXT // 2, first, second)

        across.start()
        for r in range(ROUND):
            up_buf[slot, pl.ds(r * TILE_W, TILE_W), :] = read(aligned((ROUND + r) * WIDE + own_at), TILE_W)
            down_buf[slot, pl.ds(r * TILE_W, TILE_W), :] = read(aligned((TILE_H + r) * WIDE + own_at), TILE_W)

        @pl.when(has_up)
        def _():
            up.start()
            across_up.start()

        @pl.when(has_down)
        def _():
            down.start()
            across_down.start()

    def receive(slot, write):
        up, down, across, across_up, across_down = copies(slot)

        @pl.when(has_up)
        def _():
            up.wait_send()
            across_up.wait_send()
            down.wait_recv()
            across_down.wait_recv()
            for r in range(ROUND):
                write(aligned(r * WIDE + own_at), from_up[slot, pl.ds(r * TILE_W, TILE_W), :])

        @pl.when(has_down)
        def _():
            down.wait_send()
            across_down.wait_send()
            up.wait_recv()
            across_up.wait_recv()
            for r in range(ROUND):
                write(aligned((ROUND + TILE_H + r) * WIDE + own_at), from_down[slot, pl.ds(r * TILE_W, TILE_W), :])

        across.wait_send()
        across.wait_recv()

        @pl.loop(0, ROWS // 2, unroll=10)
        def _(y):
            got = from_edge[slot, pl.ds(aligned(y * EXT), EXT), :]
            turned = pltpu.roll(got, EXT // 2, 0)
            at = 2 * y * WIDE + halo_at
            write(aligned(at), jnp.where(is_left, got, turned))
            write(aligned(at + WIDE), jnp.where(is_left, turned, got))

    def cells_of(buf, s):
        def read(at, cells):
            return buf[s, pl.ds(at, cells), :]

        def write(at, value):
            buf[s, pl.ds(at, value.shape[0]), :] = value

        return read, write

    def frames_io(s):
        return cells_of(g_buf, s)

    def state_io(s):
        return cells_of(s_buf, s)

    def frames_slot(s):
        return 2 * SAMPLES + s

    for s in range(SAMPLES):
        @pl.loop(0, TILE_H, unroll=2)
        def _(y):
            at = aligned((ROUND + y) * WIDE + own_at)
            frames_io(s)[1](at, frames_ref[s, y, :, :].astype(F32))

        send(frames_slot(s), frames_io(s)[0])

        @pl.loop(0, TILE_H, unroll=2)
        def _(y):
            at = aligned((ROUND + y) * WIDE + own_at)
            state = jnp.concatenate([h_ref[s, y, :, :].astype(F32), c_ref[s, y, :, :]], axis=1)
            state_io(s)[1](at, state)

        send(2 * s, state_io(s)[0])

    def interleaved(buf, s, y):
        return jnp.concatenate([buf[s, pl.ds(y * WIDE + v, 8, PHASES), :] for v in range(PHASES)])

    def before(value):
        first = jnp.where(cell == 0, 0.0, pltpu.roll(value[WIDE - 8:WIDE, :], 1, 0))
        return jnp.concatenate([first, value[0:WIDE - 8, :]])

    def after(value):
        last = jnp.where(cell == 7, 0.0, pltpu.roll(value[0:8, :], 7, 0))
        return jnp.concatenate([value[8:WIDE, :], last])

    def operand(value):
        return jnp.concatenate([value, tail]).astype(BF16)

    def build(s, n, y):
        state = interleaved(s_buf, s, y)
        turned = pltpu.roll(state, HALF, 1)
        c_buf[s, pl.ds(aligned(y * WIDE), WIDE), :] = turned
        frames = interleaved(g_buf, s, y)

        def frames_to(lane):
            return pltpu.roll(frames, lax.rem(lane + LANES - ROUND * C_IN * n, LANES), 1)

        lane = lane_of(WIDE)
        right = after(jnp.where(low(WIDE), state, frames_to(64)))
        second = jnp.where(lane < 80, right, jnp.where(lane < 96, frames_to(80), before(frames_to(96))))
        second = operand(second)
        to = pl.ds(pl.multiple_of(y * PITCH, PITCH), PITCH)
        a_buf[0, to, 0:LANES] = operand(jnp.where(low(WIDE), state, before(turned)))
        a_buf[0, to, LANES:2 * LANES] = second
        a_buf[1, to, LANES:2 * LANES] = second

    def advance(s, t, j):
        step = j - 1
        old, new = step % 2, 1 - step % 2
        gain = jnp.where(low(1), 0.5, 1.0)
        shift = jnp.where(low(1), 0.5, 0.0)
        for top in range(j, ROWS - j, SUB_ROWS):
            count = min(SUB_ROWS, ROWS - j - top)
            gates = None
            for dy in range(3):
                left = a_buf[old, pl.ds((top + dy - 1) * PITCH, count * PITCH), :]
                term = jnp.dot(left, w_ref[step, dy, :, :], preferred_element_type=F32)
                gates = term if gates is None else gates + term
            for r in range(count):
                y = top + r
                part = slice(r * PITCH, r * PITCH + WIDE)
                here = pl.ds(y * WIDE, WIDE)
                first = jnp.tanh(gates[part, 0:LANES] + bias_ref[0:1, :])
                second = jnp.tanh(gates[part, LANES:] + bias_ref[1:2, :])
                mixed = (0.5 * first + 0.5) * jnp.where(low(WIDE), c_buf[s, here, :], second)
                c_next = mixed + pltpu.roll(mixed, HALF, 1)
                h_next = (second * gain + shift) * jnp.tanh(c_next)
                if y < ROUND:
                    h_next = h_next * up_keep
                elif y >= ROUND + TILE_H:
                    h_next = h_next * down_keep
                else:
                    state = h_next if j < ROUND else jnp.where(low(WIDE), h_next, c_next)
                    for v in range(PHASES):
                        s_buf[s, pl.ds(y * WIDE + v, 8, PHASES), :] = state[8 * v:8 * v + 8, :]
                    own = s_buf[s, pl.ds(aligned(y * WIDE + own_at), TILE_W), :]
                    seq_ref[t, s, y - ROUND, :, :] = own[:, 0:C_HID].astype(BF16)
                if j < ROUND:
                    c_buf[s, here, :] = c_next
                    to = pl.ds(y * PITCH, PITCH)
                    side = jnp.where(low(WIDE), h_next, before(pltpu.roll(h_next, HALF, 1)))
                    a_buf[new, to, 0:LANES] = operand(side)
                    a_buf[new, to, LANES:LANES + HALF] = operand(after(h_next))[:, 0:HALF]

    for s in range(SAMPLES):
        receive(frames_slot(s), frames_io(s)[1])

    @pl.loop(0, SAMPLES * ROUNDS)
    def _(turn):
        s = lax.rem(turn, SAMPLES)
        n = lax.div(turn, SAMPLES)
        receive(2 * s + lax.rem(n, 2), state_io(s)[1])

        @pl.loop(0, ROWS, unroll=4)
        def _(y):
            build(s, n, y)

        for j in range(1, ROUND + 1):
            advance(s, ROUND * n + j - 1, j)

        @pl.when(n < ROUNDS - 1)
        def _():
            send(2 * s + lax.rem(n + 1, 2), state_io(s)[0])

    for s in range(SAMPLES):
        @pl.loop(0, TILE_H, unroll=2)
        def _(y):
            at = aligned((ROUND + y) * WIDE + own_at)
            c_out_ref[s, y, :, :] = s_buf[s, pl.ds(at, TILE_W), :][:, HALF:]


def pack_weights(w_in, w_rec):
    def gates(w):
        i, f, o, g = jnp.split(w, 4, axis=-1)
        half = jnp.asarray(0.5, w.dtype)
        return jnp.concatenate([f * half, i * half, o * half, g], axis=-1)

    rec = gates(w_rec)
    rec = jnp.concatenate([rec[:, 1], rec[:, 0], rec[:, 2]], axis=1)
    inp = gates(w_in)[:, ::-1]
    rest = LANES - HALF - 3 * ROUND * C_IN
    packed = []
    for step in range(ROUND):
        spread = jnp.pad(inp, ((0, 0), (0, 0), (step * C_IN, (ROUND - 1 - step) * C_IN), (0, 0)))
        spread = spread.reshape(3, 3 * ROUND * C_IN, 4 * C_HID)
        packed.append(jnp.concatenate([rec, jnp.pad(spread, ((0, 0), (0, rest), (0, 0)))], axis=1))
    return jnp.stack(packed)


def pack_bias(bias):
    i, f, o, g = jnp.split(bias, 4)
    return jnp.stack([jnp.concatenate([f, i]) * 0.5, jnp.concatenate([o * 0.5, g])])


def solution(mesh):
    assert mesh.shape["cols"] == 2
    seq_spec = P(None, "dp", "rows", "cols", None)
    state_spec = P("dp", "rows", "cols", None)

    def local_run(frames, w_in, w_rec, gate_bias, h_init, c_init):
        frames_cells = frames.transpose(1, 2, 3, 0, 4).reshape(SAMPLES, TILE_H, TILE_W, STEPS * C_IN)
        vmem = pl.BlockSpec(memory_space=pltpu.VMEM)
        return pl.pallas_call(
            kernel,
            out_shape=(
                pltpu.VMEM((STEPS, SAMPLES, TILE_H, TILE_W, C_HID), BF16),
                jax.ShapeDtypeStruct((SAMPLES, TILE_H, TILE_W, C_HID), F32),
            ),
            in_specs=[vmem] * 5,
            out_specs=(vmem, vmem),
            scratch_shapes=[
                pltpu.VMEM((SAMPLES, ROWS * WIDE, LANES), F32),
                pltpu.VMEM((SAMPLES, ROWS * WIDE, LANES), F32),
                pltpu.VMEM((SAMPLES, ROWS * WIDE, LANES), F32),
                pltpu.VMEM((2, ROWS * PITCH, 2 * LANES), BF16),
                pltpu.VMEM((SLOTS, STRIP, LANES), F32),
                pltpu.VMEM((SLOTS, STRIP, LANES), F32),
                pltpu.VMEM((SLOTS, EDGE, LANES), F32),
                pltpu.VMEM((SLOTS, STRIP, LANES), F32),
                pltpu.VMEM((SLOTS, STRIP, LANES), F32),
                pltpu.VMEM((SLOTS, EDGE_HALO, LANES), F32),
                pltpu.SemaphoreType.DMA((SLOTS, 5)),
                pltpu.SemaphoreType.DMA((SLOTS, 5)),
            ],
            compiler_params=pltpu.CompilerParams(
                collective_id=0, has_side_effects=True, vmem_limit_bytes=32 * 1024 * 1024),
            name="convlstm",
        )(frames_cells, h_init, c_init, pack_weights(w_in, w_rec), pack_bias(gate_bias))

    return jax.shard_map(
        local_run, mesh=mesh, in_specs=(seq_spec, P(), P(), P(), state_spec, state_spec),
        out_specs=(seq_spec, state_spec), check_vma=False)
```

```python
import jax
import jax.numpy as jnp
from jax import lax
from jax.experimental import pallas as pl
from jax.experimental.pallas import tpu as pltpu
from jax.sharding import PartitionSpec as P

MESH = pl.DeviceIdType.MESH
F32, BF16 = jnp.float32, jnp.bfloat16

STEPS = 32
SAMPLES = 2
TILE_H = 32
TILE_W = 48
C_IN = 4
C_HID = 64
ROUND = 4
ROUNDS = STEPS // ROUND
EXT = 8
WIDE = TILE_W + EXT
PHASES = WIDE // 8
PITCH = 64
SUB_ROWS = 8
ROWS = TILE_H + 2 * ROUND
LANES = 128
HALF = LANES // 2
STRIP = ROUND * TILE_W
EDGE = TILE_H // 2 * EXT
EDGE_HALO = ROWS // 2 * EXT
CORNER = ROUND // 2 * EXT
SLOTS = 3 * SAMPLES


def kernel(frames_ref, h_ref, c_ref, w_in_ref, w_rec_ref, bias_in_ref, seq_ref, c_out_ref,
           w_ref, bias_ref, s_buf, c_buf, g_buf, a_buf,
           up_buf, down_buf, edge_buf, from_up, from_down, from_edge,
           send_sem, recv_sem):
    row = lax.axis_index("rows")
    col = lax.axis_index("cols")
    has_up = row > 0
    has_down = row < lax.axis_size("rows") - 1
    is_left = col == 0
    other = 1 - col

    own_at = jnp.where(is_left, 0, EXT)
    edge_at = jnp.where(is_left, TILE_W - EXT, EXT)
    halo_at = jnp.where(is_left, TILE_W, 0)
    up_keep = has_up.astype(F32)
    down_keep = has_down.astype(F32)

    def lane_of(cells):
        return lax.broadcasted_iota(jnp.int32, (cells, LANES), 1)

    def low(cells):
        return lane_of(cells) < HALF

    def aligned(at):
        return pl.multiple_of(at, EXT)

    zero = jnp.zeros((WIDE, LANES), F32)
    tail = jnp.zeros((PITCH - WIDE, LANES), F32)

    @pl.loop(0, ROWS)
    def _(y):
        for s in range(SAMPLES):
            at = pl.ds(aligned(y * WIDE), WIDE)
            s_buf[s, at, :] = zero
            g_buf[s, at, :] = zero

    for slot in range(SLOTS):
        for at in (0, EDGE_HALO - CORNER):
            from_edge[slot, pl.ds(at, CORNER), :] = jnp.zeros((CORNER, LANES), F32)

    def gates_of(value):
        rows = value.shape[0]
        first = pltpu.roll(value[:, 0:LANES], HALF, 1) * 0.5
        second = value[:, LANES:] * jnp.where(low(rows), 0.5, 1.0)
        return first, second

    bias_ref[0:1, :], bias_ref[1:2, :] = gates_of(bias_in_ref[:, :])
    span = ROUND * C_IN
    which = lax.broadcasted_iota(jnp.int32, (span, LANES), 0) // C_IN
    for dy in range(3):
        for place, dx in enumerate((1, 0, 2)):
            for half, part in enumerate(gates_of(w_rec_ref[dy, dx, :, :].astype(F32))):
                for step in range(ROUND):
                    w_ref[step, dy, place * C_HID:(place + 1) * C_HID, half * LANES:(half + 1) * LANES] = part.astype(BF16)
        for place, dx in enumerate((2, 1, 0)):
            at = 3 * C_HID + place * span
            rows = jnp.concatenate([w_in_ref[dy, dx, :, :].astype(F32)] * ROUND)
            for half, part in enumerate(gates_of(rows)):
                for step in range(ROUND):
                    w_ref[step, dy, at:at + span, half * LANES:(half + 1) * LANES] = jnp.where(which == step, part, 0.0).astype(BF16)
        for step in range(ROUND):
            rest = 2 * LANES - 3 * (C_HID + span)
            w_ref[step, dy, 2 * LANES - rest:2 * LANES, :] = jnp.zeros((rest, 2 * LANES), BF16)

    barrier = pltpu.get_barrier_semaphore()

    def greet(target):
        pl.semaphore_signal(barrier, inc=1, device_id=target, device_id_type=MESH)

    greet({"cols": other})

    @pl.when(has_up)
    def _():
        greet({"rows": row - 1})
        greet({"rows": row - 1, "cols": other})

    @pl.when(has_down)
    def _():
        greet({"rows": row + 1})
        greet({"rows": row + 1, "cols": other})

    pl.semaphore_wait(barrier, 1 + 2 * has_up.astype(jnp.int32) + 2 * has_down.astype(jnp.int32))

    def copies(slot):
        def copy(src, dst, index, target):
            return pltpu.make_async_remote_copy(
                src_ref=src, dst_ref=dst, send_sem=send_sem.at[slot, index],
                recv_sem=recv_sem.at[slot, index], device_id=target, device_id_type=MESH)

        edge = edge_buf.at[slot]
        halo = from_edge.at[slot]
        return (
            copy(up_buf.at[slot], from_down.at[slot], 0, {"rows": row - 1}),
            copy(down_buf.at[slot], from_up.at[slot], 1, {"rows": row + 1}),
            copy(edge, halo.at[pl.ds(CORNER, EDGE)], 2, {"cols": other}),
            copy(edge.at[pl.ds(0, CORNER)], halo.at[pl.ds(CORNER + EDGE, CORNER)], 3, {"rows": row - 1, "cols": other}),
            copy(edge.at[pl.ds(EDGE - CORNER, CORNER)], halo.at[pl.ds(0, CORNER)], 4, {"rows": row + 1, "cols": other}),
        )

    cell = lax.broadcasted_iota(jnp.int32, (EXT, LANES), 0)

    def send(slot, read):
        up, down, across, across_up, across_down = copies(slot)

        @pl.loop(0, TILE_H // 2, unroll=8)
        def _(y):
            at = (ROUND + 2 * y) * WIDE + edge_at
            first = read(aligned(at), EXT)
            second = read(aligned(at + WIDE), EXT)
            first = jnp.where(is_left, pltpu.roll(first, EXT // 2, 0), first)
            second = jnp.where(is_left, second, pltpu.roll(second, EXT // 2, 0))
            edge_buf[slot, pl.ds(aligned(y * EXT), EXT), :] = jnp.where(cell < EXT // 2, first, second)

        across.start()
        for r in range(ROUND):
            up_buf[slot, pl.ds(r * TILE_W, TILE_W), :] = read(aligned((ROUND + r) * WIDE + own_at), TILE_W)
            down_buf[slot, pl.ds(r * TILE_W, TILE_W), :] = read(aligned((TILE_H + r) * WIDE + own_at), TILE_W)

        @pl.when(has_up)
        def _():
            up.start()
            across_up.start()

        @pl.when(has_down)
        def _():
            down.start()
            across_down.start()

    def receive(slot, write):
        up, down, across, across_up, across_down = copies(slot)

        @pl.when(has_up)
        def _():
            up.wait_send()
            across_up.wait_send()
            down.wait_recv()
            across_down.wait_recv()
            for r in range(ROUND):
                write(aligned(r * WIDE + own_at), from_up[slot, pl.ds(r * TILE_W, TILE_W), :])

        @pl.when(has_down)
        def _():
            down.wait_send()
            across_down.wait_send()
            up.wait_recv()
            across_up.wait_recv()
            for r in range(ROUND):
                write(aligned((ROUND + TILE_H + r) * WIDE + own_at), from_down[slot, pl.ds(r * TILE_W, TILE_W), :])

        across.wait_send()
        across.wait_recv()

        @pl.loop(0, ROWS // 2, unroll=10)
        def _(y):
            got = from_edge[slot, pl.ds(aligned(y * EXT), EXT), :]
            turned = pltpu.roll(got, EXT // 2, 0)
            at = 2 * y * WIDE + halo_at
            write(aligned(at), jnp.where(is_left, got, turned))
            write(aligned(at + WIDE), jnp.where(is_left, turned, got))

    def cells_of(buf, s):
        def read(at, cells):
            return buf[s, pl.ds(at, cells), :]

        def write(at, value):
            buf[s, pl.ds(at, value.shape[0]), :] = value

        return read, write

    def frames_io(s):
        return cells_of(g_buf, s)

    def state_io(s):
        return cells_of(s_buf, s)

    def frames_slot(s):
        return 2 * SAMPLES + s

    for s in range(SAMPLES):
        @pl.loop(0, TILE_H, unroll=2)
        def _(y):
            at = aligned((ROUND + y) * WIDE + own_at)
            frames_io(s)[1](at, frames_ref[s, y, :, :].astype(F32))

        send(frames_slot(s), frames_io(s)[0])

        @pl.loop(0, TILE_H, unroll=2)
        def _(y):
            at = aligned((ROUND + y) * WIDE + own_at)
            state = jnp.concatenate([h_ref[s, y, :, :].astype(F32), c_ref[s, y, :, :]], axis=1)
            state_io(s)[1](at, state)

        send(2 * s, state_io(s)[0])

    def interleaved(buf, s, y):
        return jnp.concatenate([buf[s, pl.ds(y * WIDE + v, 8, PHASES), :] for v in range(PHASES)])

    def before(value):
        first = jnp.where(cell == 0, 0.0, pltpu.roll(value[WIDE - 8:WIDE, :], 1, 0))
        return jnp.concatenate([first, value[0:WIDE - 8, :]])

    def after(value):
        last = jnp.where(cell == 7, 0.0, pltpu.roll(value[0:8, :], 7, 0))
        return jnp.concatenate([value[8:WIDE, :], last])

    def operand(value):
        return jnp.concatenate([value, tail]).astype(BF16)

    def build(s, n, y):
        state = interleaved(s_buf, s, y)
        turned = pltpu.roll(state, HALF, 1)
        c_buf[s, pl.ds(y * WIDE, WIDE), :] = turned
        frames = interleaved(g_buf, s, y)

        def frames_to(lane):
            return pltpu.roll(frames, lax.rem(lane + LANES - ROUND * C_IN * n, LANES), 1)

        lane = lane_of(WIDE)
        right = after(jnp.where(low(WIDE), state, frames_to(64)))
        second = jnp.where(lane < 80, right, jnp.where(lane < 96, frames_to(80), before(frames_to(96))))
        second = operand(second)
        to = pl.ds(y * PITCH, PITCH)
        a_buf[0, to, 0:LANES] = operand(jnp.where(low(WIDE), state, before(turned)))
        a_buf[0, to, LANES:2 * LANES] = second
        a_buf[1, to, LANES:2 * LANES] = second

    def advance(s, n, j):
        step = j - 1
        t = ROUND * n + step
        built = 0
        old, new = step % 2, 1 - step % 2
        gain = jnp.where(low(1), 0.5, 1.0)
        shift = jnp.where(low(1), 0.5, 0.0)
        for top in range(j, ROWS - j, SUB_ROWS):
            count = min(SUB_ROWS, ROWS - j - top)
            if j == 1:
                reach = min(top + count + 1, ROWS)
                for y in range(built, reach):
                    build(s, n, y)
                built = reach
            gates = None
            for dy in range(3):
                left = a_buf[old, pl.ds((top + dy - 1) * PITCH, count * PITCH), :]
                term = jnp.dot(left, w_ref[step, dy, :, :], preferred_element_type=F32)
                gates = term if gates is None else gates + term
            for r in range(count):
                y = top + r
                part = slice(r * PITCH, r * PITCH + WIDE)
                here = pl.ds(y * WIDE, WIDE)
                first = jnp.tanh(gates[part, 0:LANES] + bias_ref[0:1, :])
                second = jnp.tanh(gates[part, LANES:] + bias_ref[1:2, :])
                mixed = (0.5 * first + 0.5) * jnp.where(low(WIDE), c_buf[s, here, :], second)
                c_next = mixed + pltpu.roll(mixed, HALF, 1)
                h_next = (second * gain + shift) * jnp.tanh(c_next)
                if y < ROUND:
                    h_next = h_next * up_keep
                elif y >= ROUND + TILE_H:
                    h_next = h_next * down_keep
                else:
                    state = h_next if j < ROUND else jnp.where(low(WIDE), h_next, c_next)
                    for v in range(PHASES):
                        s_buf[s, pl.ds(y * WIDE + v, 8, PHASES), :] = state[8 * v:8 * v + 8, :]
                    own = s_buf[s, pl.ds(aligned(y * WIDE + own_at), TILE_W), :]
                    seq_ref[t, s, y - ROUND, :, :] = own[:, 0:C_HID].astype(BF16)
                if j < ROUND:
                    c_buf[s, here, :] = c_next
                    to = pl.ds(y * PITCH, PITCH)
                    side = jnp.where(low(WIDE), h_next, before(pltpu.roll(h_next, HALF, 1)))
                    a_buf[new, to, 0:LANES] = operand(side)
                    a_buf[new, to, LANES:LANES + HALF] = operand(after(h_next))[:, 0:HALF]

    for s in range(SAMPLES):
        receive(frames_slot(s), frames_io(s)[1])

    @pl.loop(0, SAMPLES * ROUNDS)
    def _(turn):
        s = lax.rem(turn, SAMPLES)
        n = lax.div(turn, SAMPLES)
        receive(2 * s + lax.rem(n, 2), state_io(s)[1])

        for j in range(1, ROUND + 1):
            advance(s, n, j)

        @pl.when(n < ROUNDS - 1)
        def _():
            send(2 * s + lax.rem(n + 1, 2), state_io(s)[0])

    for s in range(SAMPLES):
        @pl.loop(0, TILE_H, unroll=2)
        def _(y):
            at = aligned((ROUND + y) * WIDE + own_at)
            c_out_ref[s, y, :, :] = s_buf[s, pl.ds(at, TILE_W), :][:, HALF:]


def solution(mesh):
    assert mesh.shape["cols"] == 2
    seq_spec = P(None, "dp", "rows", "cols", None)
    state_spec = P("dp", "rows", "cols", None)

    def local_run(frames, w_in, w_rec, gate_bias, h_init, c_init):
        frames_cells = frames.transpose(1, 2, 3, 0, 4).reshape(SAMPLES, TILE_H, TILE_W, STEPS * C_IN)
        vmem = pl.BlockSpec(memory_space=pltpu.VMEM)
        return pl.pallas_call(
            kernel,
            out_shape=(
                pltpu.VMEM((STEPS, SAMPLES, TILE_H, TILE_W, C_HID), BF16),
                jax.ShapeDtypeStruct((SAMPLES, TILE_H, TILE_W, C_HID), F32),
            ),
            in_specs=[vmem] * 6,
            out_specs=(vmem, vmem),
            scratch_shapes=[
                pltpu.VMEM((ROUND, 3, 2 * LANES, 4 * C_HID), BF16),
                pltpu.VMEM((2, LANES), F32),
                pltpu.VMEM((SAMPLES, ROWS * WIDE, LANES), F32),
                pltpu.VMEM((SAMPLES, ROWS * WIDE, LANES), F32),
                pltpu.VMEM((SAMPLES, ROWS * WIDE, LANES), F32),
                pltpu.VMEM((2, ROWS * PITCH, 2 * LANES), BF16),
                pltpu.VMEM((SLOTS, STRIP, LANES), F32),
                pltpu.VMEM((SLOTS, STRIP, LANES), F32),
                pltpu.VMEM((SLOTS, EDGE, LANES), F32),
                pltpu.VMEM((SLOTS, STRIP, LANES), F32),
                pltpu.VMEM((SLOTS, STRIP, LANES), F32),
                pltpu.VMEM((SLOTS, EDGE_HALO, LANES), F32),
                pltpu.SemaphoreType.DMA((SLOTS, 5)),
                pltpu.SemaphoreType.DMA((SLOTS, 5)),
            ],
            compiler_params=pltpu.CompilerParams(
                collective_id=0, has_side_effects=True, vmem_limit_bytes=32 * 1024 * 1024),
            name="convlstm",
        )(frames_cells, h_init, c_init, w_in, w_rec, gate_bias.reshape(1, 4 * C_HID))

    return jax.shard_map(
        local_run, mesh=mesh, in_specs=(seq_spec, P(), P(), P(), state_spec, state_spec),
        out_specs=(seq_spec, state_spec), check_vma=False)
```

```python
import jax
import jax.numpy as jnp
from jax import lax
from jax.experimental import pallas as pl
from jax.experimental.pallas import tpu as pltpu
from jax.sharding import PartitionSpec as P

MESH = pl.DeviceIdType.MESH
F32, BF16 = jnp.float32, jnp.bfloat16

STEPS = 32
SAMPLES = 2
TILE_H = 32
TILE_W = 48
C_IN = 4
C_HID = 64
ROUND = 4
ROUNDS = STEPS // ROUND
EXT = 8
WIDE = TILE_W + EXT
PHASES = WIDE // 8
PITCH = 64
GROUPS = ((4, 8, 8, 8, 8, 2), (8, 8, 8, 8, 4), (8, 8, 8, 8, 2), (8, 8, 8, 8))
ROWS = TILE_H + 2 * ROUND
LANES = 128
HALF = LANES // 2
STRIP = ROUND * TILE_W
EDGE = TILE_H // 2 * EXT
EDGE_HALO = ROWS // 2 * EXT
CORNER = ROUND // 2 * EXT
SLOTS = 3 * SAMPLES


def kernel(frames_ref, h_ref, c_ref, w_in_ref, w_rec_ref, bias_in_ref, seq_ref, c_out_ref,
           w_ref, bias_ref, s_buf, c_buf, g_buf, f_buf, a_buf,
           up_buf, down_buf, edge_buf, from_up, from_down, from_edge,
           send_sem, recv_sem):
    row = lax.axis_index("rows")
    col = lax.axis_index("cols")
    has_up = row > 0
    has_down = row < lax.axis_size("rows") - 1
    is_left = col == 0
    other = 1 - col

    own_at = jnp.where(is_left, 0, EXT)
    edge_at = jnp.where(is_left, TILE_W - EXT, EXT)
    halo_at = jnp.where(is_left, TILE_W, 0)
    up_keep = has_up.astype(F32)
    down_keep = has_down.astype(F32)

    def lane_of(cells):
        return lax.broadcasted_iota(jnp.int32, (cells, LANES), 1)

    def low(cells):
        return lane_of(cells) < HALF

    def aligned(at):
        return pl.multiple_of(at, EXT)

    zero = jnp.zeros((WIDE, LANES), F32)
    tail = jnp.zeros((PITCH - WIDE, LANES), F32)

    @pl.loop(0, ROWS)
    def _(y):
        for s in range(SAMPLES):
            at = pl.ds(aligned(y * WIDE), WIDE)
            s_buf[s, at, :] = zero
            g_buf[s, at, :] = zero

    for slot in range(SLOTS):
        for at in (0, EDGE_HALO - CORNER):
            from_edge[slot, pl.ds(at, CORNER), :] = jnp.zeros((CORNER, LANES), F32)

    def gates_of(value):
        rows = value.shape[0]
        first = pltpu.roll(value[:, 0:LANES], HALF, 1) * 0.5
        second = value[:, LANES:] * jnp.where(low(rows), 0.5, 1.0)
        return first, second

    bias_ref[0:1, :], bias_ref[1:2, :] = gates_of(bias_in_ref[:, :])
    span = ROUND * C_IN
    which = lax.broadcasted_iota(jnp.int32, (span, LANES), 0) // C_IN
    for dy in range(3):
        for place, dx in enumerate((1, 0, 2)):
            for half, part in enumerate(gates_of(w_rec_ref[dy, dx, :, :].astype(F32))):
                for step in range(ROUND):
                    w_ref[step, dy, place * C_HID:(place + 1) * C_HID, half * LANES:(half + 1) * LANES] = part.astype(BF16)
        for place, dx in enumerate((2, 1, 0)):
            at = 3 * C_HID + place * span
            rows = jnp.concatenate([w_in_ref[dy, dx, :, :].astype(F32)] * ROUND)
            for half, part in enumerate(gates_of(rows)):
                for step in range(ROUND):
                    w_ref[step, dy, at:at + span, half * LANES:(half + 1) * LANES] = jnp.where(which == step, part, 0.0).astype(BF16)
        for step in range(ROUND):
            rest = 2 * LANES - 3 * (C_HID + span)
            w_ref[step, dy, 2 * LANES - rest:2 * LANES, :] = jnp.zeros((rest, 2 * LANES), BF16)

    barrier = pltpu.get_barrier_semaphore()

    def greet(target):
        pl.semaphore_signal(barrier, inc=1, device_id=target, device_id_type=MESH)

    greet({"cols": other})

    @pl.when(has_up)
    def _():
        greet({"rows": row - 1})
        greet({"rows": row - 1, "cols": other})

    @pl.when(has_down)
    def _():
        greet({"rows": row + 1})
        greet({"rows": row + 1, "cols": other})

    pl.semaphore_wait(barrier, 1 + 2 * has_up.astype(jnp.int32) + 2 * has_down.astype(jnp.int32))

    def copies(slot):
        def copy(src, dst, index, target):
            return pltpu.make_async_remote_copy(
                src_ref=src, dst_ref=dst, send_sem=send_sem.at[slot, index],
                recv_sem=recv_sem.at[slot, index], device_id=target, device_id_type=MESH)

        edge = edge_buf.at[slot]
        halo = from_edge.at[slot]
        return (
            copy(up_buf.at[slot], from_down.at[slot], 0, {"rows": row - 1}),
            copy(down_buf.at[slot], from_up.at[slot], 1, {"rows": row + 1}),
            copy(edge, halo.at[pl.ds(CORNER, EDGE)], 2, {"cols": other}),
            copy(edge.at[pl.ds(0, CORNER)], halo.at[pl.ds(CORNER + EDGE, CORNER)], 3, {"rows": row - 1, "cols": other}),
            copy(edge.at[pl.ds(EDGE - CORNER, CORNER)], halo.at[pl.ds(0, CORNER)], 4, {"rows": row + 1, "cols": other}),
        )

    cell = lax.broadcasted_iota(jnp.int32, (EXT, LANES), 0)

    def send(slot, read):
        up, down, across, across_up, across_down = copies(slot)

        @pl.loop(0, TILE_H // 2, unroll=8)
        def _(y):
            at = (ROUND + 2 * y) * WIDE + edge_at
            first = read(aligned(at), EXT)
            second = read(aligned(at + WIDE), EXT)
            first = jnp.where(is_left, pltpu.roll(first, EXT // 2, 0), first)
            second = jnp.where(is_left, second, pltpu.roll(second, EXT // 2, 0))
            edge_buf[slot, pl.ds(aligned(y * EXT), EXT), :] = jnp.where(cell < EXT // 2, first, second)

        across.start()
        for r in range(ROUND):
            up_buf[slot, pl.ds(r * TILE_W, TILE_W), :] = read(aligned((ROUND + r) * WIDE + own_at), TILE_W)
            down_buf[slot, pl.ds(r * TILE_W, TILE_W), :] = read(aligned((TILE_H + r) * WIDE + own_at), TILE_W)

        @pl.when(has_up)
        def _():
            up.start()
            across_up.start()

        @pl.when(has_down)
        def _():
            down.start()
            across_down.start()

    def receive(slot, write):
        up, down, across, across_up, across_down = copies(slot)

        @pl.when(has_up)
        def _():
            up.wait_send()
            across_up.wait_send()
            down.wait_recv()
            across_down.wait_recv()
            for r in range(ROUND):
                write(aligned(r * WIDE + own_at), from_up[slot, pl.ds(r * TILE_W, TILE_W), :])

        @pl.when(has_down)
        def _():
            down.wait_send()
            across_down.wait_send()
            up.wait_recv()
            across_up.wait_recv()
            for r in range(ROUND):
                write(aligned((ROUND + TILE_H + r) * WIDE + own_at), from_down[slot, pl.ds(r * TILE_W, TILE_W), :])

        across.wait_send()
        across.wait_recv()

        @pl.loop(0, ROWS // 2, unroll=10)
        def _(y):
            got = from_edge[slot, pl.ds(aligned(y * EXT), EXT), :]
            turned = pltpu.roll(got, EXT // 2, 0)
            at = 2 * y * WIDE + halo_at
            write(aligned(at), jnp.where(is_left, got, turned))
            write(aligned(at + WIDE), jnp.where(is_left, turned, got))

    def cells_of(buf, s):
        def read(at, cells):
            return buf[s, pl.ds(at, cells), :]

        def write(at, value):
            buf[s, pl.ds(at, value.shape[0]), :] = value

        return read, write

    def frames_io(s):
        return cells_of(g_buf, s)

    def state_io(s):
        return cells_of(s_buf, s)

    def frames_slot(s):
        return 2 * SAMPLES + s

    for s in range(SAMPLES):
        @pl.loop(0, TILE_H, unroll=2)
        def _(y):
            at = aligned((ROUND + y) * WIDE + own_at)
            frames_io(s)[1](at, frames_ref[s, y, :, :].astype(F32))

        send(frames_slot(s), frames_io(s)[0])

        @pl.loop(0, TILE_H, unroll=2)
        def _(y):
            at = aligned((ROUND + y) * WIDE + own_at)
            state = jnp.concatenate([h_ref[s, y, :, :].astype(F32), c_ref[s, y, :, :]], axis=1)
            state_io(s)[1](at, state)

        send(2 * s, state_io(s)[0])

    def interleaved(buf, s, y):
        return jnp.concatenate([buf[s, pl.ds(y * WIDE + v, 8, PHASES), :] for v in range(PHASES)])

    def before(value):
        first = jnp.where(cell == 0, 0.0, pltpu.roll(value[WIDE - 8:WIDE, :], 1, 0))
        return jnp.concatenate([first, value[0:WIDE - 8, :]])

    def after(value):
        last = jnp.where(cell == 7, 0.0, pltpu.roll(value[0:8, :], 7, 0))
        return jnp.concatenate([value[8:WIDE, :], last])

    def operand(value):
        return jnp.concatenate([value, tail]).astype(BF16)

    span_lanes = ROUND * C_IN

    def lay_frames(s, y):
        frames = interleaved(g_buf, s, y)
        to = pl.ds(pl.multiple_of(y * PITCH, PITCH), PITCH)
        f_buf[0, s, to, :] = operand(after(frames))
        f_buf[1, s, to, :] = operand(pltpu.roll(frames, span_lanes, 1))
        f_buf[2, s, to, :] = operand(before(pltpu.roll(frames, 2 * span_lanes, 1)))

    def build(s, n, y):
        state = interleaved(s_buf, s, y)
        turned = pltpu.roll(state, HALF, 1)
        c_buf[s, pl.ds(y * WIDE, WIDE), :] = turned
        to = pl.ds(y * PITCH, PITCH)
        place = lax.rem(lane_of(PITCH) + (LANES - span_lanes * n), LANES).astype(BF16)
        frames = jnp.where(place < span_lanes, f_buf[0, s, to, :], jnp.where(place < 2 * span_lanes, f_buf[1, s, to, :], f_buf[2, s, to, :]))
        frames = pltpu.roll(frames, lax.rem(HALF + LANES - span_lanes * n, LANES), 1)
        a_buf[0, to, 0:LANES] = operand(jnp.where(low(WIDE), state, before(turned)))
        second = jnp.where(lane_of(PITCH).astype(BF16) < HALF, operand(after(state)), frames)
        a_buf[0, to, LANES:2 * LANES] = second
        a_buf[1, to, LANES:2 * LANES] = second

    def advance(s, n, j):
        step = j - 1
        t = ROUND * n + step
        built = 0
        old, new = step % 2, 1 - step % 2
        gain = jnp.where(low(1), 0.5, 1.0)
        shift = jnp.where(low(1), 0.5, 0.0)
        top = j
        for count in GROUPS[step]:
            if j == 1:
                reach = min(top + count + 1, ROWS)
                for y in range(built, reach):
                    build(s, n, y)
                built = reach
            gates = None
            for dy in range(3):
                left = a_buf[old, pl.ds((top + dy - 1) * PITCH, count * PITCH), :]
                term = jnp.dot(left, w_ref[step, dy, :, :], preferred_element_type=F32)
                gates = term if gates is None else gates + term
            for r in range(count):
                y = top + r
                part = slice(r * PITCH, r * PITCH + WIDE)
                here = pl.ds(y * WIDE, WIDE)
                first = jnp.tanh(gates[part, 0:LANES] + bias_ref[0:1, :])
                second = jnp.tanh(gates[part, LANES:] + bias_ref[1:2, :])
                mixed = (0.5 * first + 0.5) * jnp.where(low(WIDE), c_buf[s, here, :], second)
                c_next = mixed + pltpu.roll(mixed, HALF, 1)
                h_next = (second * gain + shift) * jnp.tanh(c_next)
                if y < ROUND:
                    h_next = h_next * up_keep
                elif y >= ROUND + TILE_H:
                    h_next = h_next * down_keep
                else:
                    state = h_next if j < ROUND else jnp.where(low(WIDE), h_next, c_next)
                    for v in range(PHASES):
                        s_buf[s, pl.ds(y * WIDE + v, 8, PHASES), :] = state[8 * v:8 * v + 8, :]
                    own = s_buf[s, pl.ds(aligned(y * WIDE + own_at), TILE_W), :]
                    seq_ref[t, s, y - ROUND, :, :] = own[:, 0:C_HID].astype(BF16)
                if j < ROUND:
                    c_buf[s, here, :] = c_next
                    to = pl.ds(y * PITCH, PITCH)
                    side = jnp.where(low(WIDE), h_next, before(pltpu.roll(h_next, HALF, 1)))
                    a_buf[new, to, 0:LANES] = operand(side)
                    a_buf[new, to, LANES:LANES + HALF] = operand(after(h_next))[:, 0:HALF]
            top += count

    for s in range(SAMPLES):
        receive(frames_slot(s), frames_io(s)[1])

        @pl.loop(0, ROWS, unroll=2)
        def _(y):
            lay_frames(s, y)

    @pl.loop(0, SAMPLES * ROUNDS)
    def _(turn):
        s = lax.rem(turn, SAMPLES)
        n = lax.div(turn, SAMPLES)
        receive(2 * s + lax.rem(n, 2), state_io(s)[1])

        for j in range(1, ROUND + 1):
            advance(s, n, j)

        @pl.when(n < ROUNDS - 1)
        def _():
            send(2 * s + lax.rem(n + 1, 2), state_io(s)[0])

    for s in range(SAMPLES):
        @pl.loop(0, TILE_H, unroll=2)
        def _(y):
            at = aligned((ROUND + y) * WIDE + own_at)
            c_out_ref[s, y, :, :] = s_buf[s, pl.ds(at, TILE_W), :][:, HALF:]


def solution(mesh):
    assert mesh.shape["cols"] == 2
    seq_spec = P(None, "dp", "rows", "cols", None)
    state_spec = P("dp", "rows", "cols", None)

    def local_run(frames, w_in, w_rec, gate_bias, h_init, c_init):
        frames_cells = frames.transpose(1, 2, 3, 0, 4).reshape(SAMPLES, TILE_H, TILE_W, STEPS * C_IN)
        vmem = pl.BlockSpec(memory_space=pltpu.VMEM)
        return pl.pallas_call(
            kernel,
            out_shape=(
                pltpu.VMEM((STEPS, SAMPLES, TILE_H, TILE_W, C_HID), BF16),
                jax.ShapeDtypeStruct((SAMPLES, TILE_H, TILE_W, C_HID), F32),
            ),
            in_specs=[vmem] * 6,
            out_specs=(vmem, vmem),
            scratch_shapes=[
                pltpu.VMEM((ROUND, 3, 2 * LANES, 4 * C_HID), BF16),
                pltpu.VMEM((2, LANES), F32),
                pltpu.VMEM((SAMPLES, ROWS * WIDE, LANES), F32),
                pltpu.VMEM((SAMPLES, ROWS * WIDE, LANES), F32),
                pltpu.VMEM((SAMPLES, ROWS * WIDE, LANES), F32),
                pltpu.VMEM((3, SAMPLES, ROWS * PITCH, LANES), BF16),
                pltpu.VMEM((2, ROWS * PITCH, 2 * LANES), BF16),
                pltpu.VMEM((SLOTS, STRIP, LANES), F32),
                pltpu.VMEM((SLOTS, STRIP, LANES), F32),
                pltpu.VMEM((SLOTS, EDGE, LANES), F32),
                pltpu.VMEM((SLOTS, STRIP, LANES), F32),
                pltpu.VMEM((SLOTS, STRIP, LANES), F32),
                pltpu.VMEM((SLOTS, EDGE_HALO, LANES), F32),
                pltpu.SemaphoreType.DMA((SLOTS, 5)),
                pltpu.SemaphoreType.DMA((SLOTS, 5)),
            ],
            compiler_params=pltpu.CompilerParams(
                collective_id=0, has_side_effects=True, vmem_limit_bytes=32 * 1024 * 1024),
            name="convlstm",
        )(frames_cells, h_init, c_init, w_in, w_rec, gate_bias.reshape(1, 4 * C_HID))

    return jax.shard_map(
        local_run, mesh=mesh, in_specs=(seq_spec, P(), P(), P(), state_spec, state_spec),
        out_specs=(seq_spec, state_spec), check_vma=False)
```
